16 devices in a mesh: dp: 1, ep: 16 (over x, y, z, core).
Axes of the slice: x: 2, y: 2, z: 2, core: 2. Of those that a mesh axis runs over, the one named last changes fastest.
Arguments:
- x: bfloat16 [1, 16, 256, 1792], P('dp', 'ep')
- expert: int32 [1, 16, 256, 2], P('dp', 'ep')
- slot: int32 [1, 16, 256, 2], P('dp', 'ep')
- gate: float32 [1, 16, 256, 2], P('dp', 'ep')
- w_gate: bfloat16 [32, 1792, 4864], P('ep')
- w_up: bfloat16 [32, 1792, 4864], P('ep')
- w_down: bfloat16 [32, 4864, 1792], P('ep')
Outputs:
- y: bfloat16 [1, 16, 256, 1792], P('dp', 'ep')
All inputs are finite; a program needn't handle non-finite values.
Results may differ from the reference program's by a relative error of at most 0.009.
Values are sent between devices in bfloat16 or wider.
A program may use at most 2 GiB of HBM per device.

```python
import jax
import jax.numpy as jnp

MEMBERS = 16
TOKENS = 256
D = 1792
FF = 4864
TOP = 2
EXPERTS = 32
SLOTS = 5 * TOKENS * TOP // (4 * EXPERTS)


def setup_inputs(seed: int = 0, part: int = 0) -> dict:
    own, k1, k2, k3, k4, k5, k6 = jax.random.split(jax.random.key(seed), 7)
    kx, ke, kl, kg = jax.random.split(jax.random.fold_in(own, part), 4)
    devices = (1, MEMBERS)
    place = jax.random.permutation(kl, jnp.arange(EXPERTS, dtype=jnp.uint32))
    slow = ((EXPERTS + (9 * place) % EXPERTS) << ((9 * place) // EXPERTS)) // EXPERTS
    wait = (jax.random.bits(ke, (*devices, TOKENS, EXPERTS), jnp.uint32) >> 10) * slow
    expert = jnp.argsort(wait, axis=-1)[..., :TOP].astype(jnp.int32)
    chosen = jax.nn.one_hot(expert, EXPERTS, dtype=jnp.int32)
    in_line = jnp.cumsum(chosen.reshape(*devices, TOKENS * TOP, EXPERTS), axis=2) - 1
    slot = jnp.sum(in_line.reshape(chosen.shape) * chosen, axis=-1)

    def one(key, rows, columns):
        return (jax.random.normal(key, (rows, columns), jnp.float32) * rows**-0.5).astype(jnp.bfloat16)

    def weights(key, rows, columns):
        return jax.lax.map(lambda k: one(k, rows, columns), jax.random.split(key, EXPERTS))

    return {
        "x": jax.random.normal(kx, (*devices, TOKENS, D), jnp.float32).astype(jnp.bfloat16),
        "expert": expert,
        "slot": slot,
        "gate": jax.nn.softmax(jax.random.normal(kg, expert.shape, jnp.float32)),
        "w_gate": weights(k1, D, FF),
        "w_up": weights(k2, D, FF),
        "w_down": weights(k3, FF, D),
    }


def einsum(form, a, b):
    return jnp.einsum(form, a.astype(jnp.float32), b.astype(jnp.float32))


def reference(x, expert, slot, gate, w_gate, w_up, w_down):
    to_expert = jax.nn.one_hot(expert, EXPERTS, dtype=jnp.bfloat16)
    to_slot = jax.nn.one_hot(slot, SLOTS, dtype=jnp.bfloat16)
    weighted = to_expert * gate[..., None].astype(jnp.bfloat16)
    dispatch = einsum("abtke,abtkc->abtec", to_expert, to_slot).astype(jnp.bfloat16)
    combine = einsum("abtke,abtkc->abtec", weighted, to_slot).astype(jnp.bfloat16)
    z = einsum("abtec,abtd->aebcd", dispatch, x).astype(jnp.bfloat16)
    h = jax.nn.silu(einsum("aebcd,edf->aebcf", z, w_gate))
    h = (h * einsum("aebcd,edf->aebcf", z, w_up)).astype(jnp.bfloat16)
    out = einsum("aebcf,efd->aebcd", h, w_down).astype(jnp.bfloat16)
    y = einsum("abtec,aebcd->abtd", combine, out)
    return y.astype(jnp.bfloat16)
```

```python
import functools

import jax
import jax.numpy as jnp
from jax import lax
from jax.experimental import pallas as pl
from jax.experimental.pallas import tpu as pltpu
from jax.sharding import PartitionSpec as P

N = 16
LOCAL = 2
T, D, F = 256, 1792, 4864
SLOTS, MAIN = 20, 16
HALF = D // 2
FT = 256
NF = F // FT
RING = 8
CHUNKS = ((0, 512), (512, 512), (1024, 512), (1536, 256))
f32, bf16, i32 = jnp.float32, jnp.bfloat16, jnp.int32


def dot(a, b):
    return jnp.dot(a, b, preferred_element_type=f32)


def iota(shape, axis):
    return lax.broadcasted_iota(i32, shape, axis)


def kernel(x_hbm, expert, slot, gate, wg_hbm, wu_hbm, wd_hbm, y_ref,
           x_v, zs, zr, lhs, h, wb, wd, os0, os1, os2, os3, cr0, cr1, cr2, cr3,
           x_sem, wb_sem, wd_sem, ds_sem, dr_sem, cs_sem, cr_sem):
    os, cr = (os0, os1, os2, os3), (cr0, cr1, cr2, cr3)
    me = lax.axis_index("ep")
    bits = [(me // (1 << b)) % 2 for b in range(4)]

    def partner(k):
        return sum((1 - bits[b] if (k >> b) & 1 else bits[b]) * (1 << b) for b in range(4))

    order = [partner((7 * k) % 16) for k in range(1, N)]

    x_copy = pltpu.make_async_copy(x_hbm, x_v, x_sem)
    x_copy.start()
    barrier = pltpu.get_barrier_semaphore()
    for d in order:
        pl.semaphore_signal(barrier, inc=1, device_id={"ep": d}, device_id_type=pl.DeviceIdType.MESH)

    def wb_copies(g):
        e, f, s = g // NF, g % NF, g % RING
        cols = pl.ds(pl.multiple_of(f * FT, FT), FT)
        return (pltpu.make_async_copy(wg_hbm.at[e, :, cols], wb.at[s, :, pl.ds(0, FT)], wb_sem.at[s]),
                pltpu.make_async_copy(wu_hbm.at[e, :, cols], wb.at[s, :, pl.ds(FT, FT)], wb_sem.at[s]))

    def wd_copy(e, c):
        cols = pl.ds(*CHUNKS[c])
        return pltpu.make_async_copy(wd_hbm.at[e, :, cols], wd.at[:, cols], wd_sem.at[c])

    col = [jnp.where(slot[:, j:j + 1] < SLOTS, expert[:, j:j + 1] * 32 + slot[:, j:j + 1], -1) for j in range(2)]
    row = [jnp.transpose(jnp.broadcast_to(c, (T, 128)))[0:1, :] for c in col]
    weight = [gate[:, j:j + 1].astype(bf16).astype(f32) for j in range(2)]

    def main_code(r, e):
        return (2 * (r >> 4) + e) * 32 + (r & 15)

    def rem_code(r, e, side):
        return jnp.where(((r >> 2) & 1) == side, (2 * (r >> 3) + e) * 32 + MAIN + (r & 3), -2)

    def pick(code):
        shape = (code.shape[0], T)
        hit = (jnp.broadcast_to(code, shape) == jnp.broadcast_to(row[0], shape)) | (
            jnp.broadcast_to(code, shape) == jnp.broadcast_to(row[1], shape))
        return jnp.where(hit, 1.0, 0.0).astype(bf16)

    def blend(code):
        shape = (T, code.shape[1])
        return sum(jnp.where(jnp.broadcast_to(col[j], shape) == jnp.broadcast_to(code, shape),
                             jnp.broadcast_to(weight[j], shape), 0.0) for j in range(2)).astype(bf16)

    x_copy.wait()
    for g in range(RING):
        for c in wb_copies(g):
            c.start()
    for c in range(len(CHUNKS)):
        wd_copy(0, c).start()

    def disp(e, d):
        return pltpu.make_async_remote_copy(
            src_ref=zs.at[e, d], dst_ref=zr.at[e, me], send_sem=ds_sem.at[e], recv_sem=dr_sem.at[e],
            device_id={"ep": d}, device_id_type=pl.DeviceIdType.MESH)

    for e in range(LOCAL):
        z = dot(pick(main_code(iota((N * MAIN, 1), 0), e)), x_v[...]).astype(bf16)
        zs[e, :, 0:16, :] = z[:, :HALF].reshape(N, 16, HALF)
        zs[e, :, 16:32, :] = z[:, HALF:].reshape(N, 16, HALF)
        r = iota((N * 8, 1), 0)
        z = dot(pick(rem_code(r, e, 0)), x_v[:, :HALF]) + dot(pick(rem_code(r, e, 1)), x_v[:, HALF:])
        zs[e, :, 32:40, :] = z.astype(bf16).reshape(N, 8, HALF)
        if e == 0:
            pl.semaphore_wait(barrier, N - 1)
        for d in order:
            disp(e, d).start()
        zr[e, me] = zs[e, me]

    fold_l = jnp.where(((iota((128, 64), 0) >> 3) * 4 + (iota((128, 64), 0) & 7)) == iota((128, 64), 1), 1.0, 0.0)
    fold_l = jnp.where((iota((128, 64), 0) & 7) < 4, fold_l, 0.0).astype(bf16)
    fold_r = jnp.where(((iota((128, 64), 0) >> 3) * 4 + (iota((128, 64), 0) & 7) - 4) == iota((128, 64), 1), 1.0, 0.0)
    fold_r = jnp.where((iota((128, 64), 0) & 7) >= 4, fold_r, 0.0).astype(bf16)
    un_r = iota((64, 128), 0)
    un_c = iota((64, 128), 1)
    unfold_l = jnp.where((un_r >> 2) * 8 + (un_r & 3) == un_c, 1.0, 0.0).astype(bf16)
    unfold_r = jnp.where((un_r >> 2) * 8 + (un_r & 3) + 4 == un_c, 1.0, 0.0).astype(bf16)

    def comb(e, c, d):
        return pltpu.make_async_remote_copy(
            src_ref=os[c].at[e, d], dst_ref=cr[c].at[e, me], send_sem=cs_sem.at[e, c], recv_sem=cr_sem.at[e, c],
            device_id={"ep": d}, device_id_type=pl.DeviceIdType.MESH)

    def landed(ref, sem):
        pltpu.make_async_copy(ref.at[pl.ds(0, N - 1)], ref.at[pl.ds(0, N - 1)], sem).wait()

    for e in range(LOCAL):
        landed(zr.at[e], dr_sem.at[e])
        lhs[0:256, :HALF] = zr[e, :, 0:16, :].reshape(N * 16, HALF)
        lhs[0:256, HALF:] = zr[e, :, 16:32, :].reshape(N * 16, HALF)
        rem = zr[e, :, 32:40, :].reshape(N * 8, HALF)
        lhs[256:320, :HALF] = dot(unfold_l, rem).astype(bf16)
        lhs[256:320, HALF:] = dot(unfold_r, rem).astype(bf16)

        @pl.loop(0, NF)
        def _(f):
            g = e * NF + f
            s = g % RING
            pltpu.make_async_copy(wb.at[s], wb.at[s], wb_sem.at[s]).wait()
            gu = dot(lhs[...], wb[s])
            h[:, pl.ds(pl.multiple_of(f * FT, FT), FT)] = (jax.nn.silu(gu[:, :FT]) * gu[:, FT:]).astype(bf16)

            @pl.when(g + RING < LOCAL * NF)
            def _():
                for c in wb_copies(g + RING):
                    c.start()

        for c, (c0, width) in enumerate(CHUNKS):
            w2 = width // 2
            wd_copy(e, c).wait()
            out = dot(h[...], wd[:, pl.ds(c0, width)]).astype(bf16)
            if e + 1 < LOCAL:
                wd_copy(e + 1, c).start()
            os[c][e, :, 0:16, :] = out[0:256, :w2].reshape(N, 16, w2)
            os[c][e, :, 16:32, :] = out[0:256, w2:].reshape(N, 16, w2)
            rem = dot(fold_l, out[256:320, :w2]) + dot(fold_r, out[256:320, w2:])
            os[c][e, :, 32:40, :] = rem.astype(bf16).reshape(N, 8, w2)
            for d in order:
                comb(e, c, d).start()
            cr[c][e, me] = os[c][e, me]

    mains = [blend(main_code(iota((1, 256), 1), e)) for e in range(LOCAL)]
    rems = [[blend(rem_code(iota((1, 128), 1), e, side)) for side in range(2)] for e in range(LOCAL)]
    for c, (c0, width) in enumerate(CHUNKS):
        w2 = width // 2
        for e in range(LOCAL):
            landed(cr[c].at[e], cr_sem.at[e, c])
        for side in range(2):
            acc = 0
            for e in range(LOCAL):
                acc += dot(mains[e], cr[c][e, :, 16 * side:16 * side + 16, :].reshape(N * 16, w2))
                acc += dot(rems[e][side], cr[c][e, :, 32:40, :].reshape(N * 8, w2))
            y_ref[:, pl.ds(c0 + side * w2, w2)] = acc.astype(bf16)

    for e in range(LOCAL):
        landed(zs.at[e], ds_sem.at[e])
        for c in range(len(CHUNKS)):
            landed(os[c].at[e], cs_sem.at[e, c])


def solution(mesh):
    def body(x, expert, slot, gate, wg, wu, wd):
        vmem = pl.BlockSpec(memory_space=pltpu.VMEM)
        hbm = pl.BlockSpec(memory_space=pltpu.HBM)
        halves = [w // 2 for _, w in CHUNKS]
        y = pl.pallas_call(
            kernel,
            name="moe",
            out_shape=jax.ShapeDtypeStruct((T, D), bf16),
            in_specs=[hbm, vmem, vmem, vmem, hbm, hbm, hbm],
            out_specs=vmem,
            scratch_shapes=[
                pltpu.VMEM((T, D), bf16),
                pltpu.VMEM((LOCAL, N, 40, HALF), bf16),
                pltpu.VMEM((LOCAL, N, 40, HALF), bf16),
                pltpu.VMEM((N * SLOTS, D), bf16),
                pltpu.VMEM((N * SLOTS, F), bf16),
                pltpu.VMEM((RING, D, 2 * FT), bf16),
                pltpu.VMEM((F, D), bf16),
                *[pltpu.VMEM((LOCAL, N, 40, w), bf16) for w in halves],
                *[pltpu.VMEM((LOCAL, N, 40, w), bf16) for w in halves],
                pltpu.SemaphoreType.DMA,
                pltpu.SemaphoreType.DMA((RING,)),
                pltpu.SemaphoreType.DMA((len(CHUNKS),)),
                pltpu.SemaphoreType.DMA((LOCAL,)),
                pltpu.SemaphoreType.DMA((LOCAL,)),
                pltpu.SemaphoreType.DMA((LOCAL, len(CHUNKS))),
                pltpu.SemaphoreType.DMA((LOCAL, len(CHUNKS))),
            ],
            compiler_params=pltpu.CompilerParams(
                collective_id=0, has_side_effects=True, vmem_limit_bytes=67_000_000),
        )(x[0, 0], expert[0, 0], slot[0, 0], gate[0, 0], wg, wu, wd)
        return y[None, None]

    tok, weights = P("dp", "ep", None, None), P("ep", None, None)
    return jax.shard_map(body, mesh=mesh, in_specs=(tok,) * 4 + (weights,) * 3, out_specs=tok, check_vma=False)
```

```python
import functools

import jax
import jax.numpy as jnp
from jax import lax
from jax.experimental import pallas as pl
from jax.experimental.pallas import tpu as pltpu
from jax.sharding import PartitionSpec as P

N = 16
LOCAL = 2
VMEM_LIMIT = 65_500_000
T, D, F = 256, 1792, 4864
SLOTS, MAIN = 20, 16
KS = ((0, 1024), (1024, 768))
FT = 256
NF = F // FT
RING, GROUP = 8, 4
CHUNKS = ((0, 512), (512, 512), (1024, 512), (1536, 256))
f32, bf16, i32 = jnp.float32, jnp.bfloat16, jnp.int32


def dot(a, b):
    return jnp.dot(a, b, preferred_element_type=f32)


def iota(shape, axis):
    return lax.broadcasted_iota(i32, shape, axis)


def kernel(x_hbm, expert, slot, gate, wg_hbm, wu_hbm, wd_hbm, y_ref,
           x_v, zs0, zs1, zr0, zr1, lhs, acc, h, wb, wd, os0, os1, os2, os3, cr0, cr1, cr2, cr3, bm, br,
           x_sem, wb_sem, wd_sem, ds_sem, dr_sem, cs_sem, cr_sem):
    zs, zr = (zs0, zs1), (zr0, zr1)
    os, cr = (os0, os1, os2, os3), (cr0, cr1, cr2, cr3)
    me = lax.axis_index("ep")
    bits = [(me // (1 << b)) % 2 for b in range(4)]

    def partner(k):
        return sum((1 - bits[b] if (k >> b) & 1 else bits[b]) * (1 << b) for b in range(4))

    order = [partner((7 * k) % 16) for k in range(1, N)]

    x_copy = pltpu.make_async_copy(x_hbm, x_v, x_sem)
    x_copy.start()
    barrier = pltpu.get_barrier_semaphore()
    for d in order:
        pl.semaphore_signal(barrier, inc=1, device_id={"ep": d}, device_id_type=pl.DeviceIdType.MESH)

    def wb_start(g, k):
        e, f, s = g // NF, g % NF, g % RING
        rows, cols = pl.ds(*KS[k]), pl.ds(pl.multiple_of(f * FT, FT), FT)
        pltpu.make_async_copy(wg_hbm.at[e, rows, cols], wb.at[s, rows, pl.ds(0, FT)], wb_sem.at[k, s]).start()
        pltpu.make_async_copy(wu_hbm.at[e, rows, cols], wb.at[s, rows, pl.ds(FT, FT)], wb_sem.at[k, s]).start()

    def wb_wait(g, k):
        part = wb.at[g % RING, pl.ds(*KS[k])]
        pltpu.make_async_copy(part, part, wb_sem.at[k, g % RING]).wait()

    def wd_copy(e, c):
        cols = pl.ds(*CHUNKS[c])
        return pltpu.make_async_copy(wd_hbm.at[e, :, cols], wd.at[:, cols], wd_sem.at[c])

    row = [jnp.where(slot[j:j + 1] < SLOTS, expert[j:j + 1] * 32 + slot[j:j + 1], -1) for j in range(2)]

    def main_code(r, e):
        return (2 * (r >> 4) + e) * 32 + (r & 15)

    def rem_code(r, e, side):
        return jnp.where(((r >> 2) & 1) == side, (2 * (r >> 3) + e) * 32 + MAIN + (r & 3), -2)

    def pick(code):
        shape = (code.shape[0], T)
        hit = (jnp.broadcast_to(code, shape) == jnp.broadcast_to(row[0], shape)) | (
            jnp.broadcast_to(code, shape) == jnp.broadcast_to(row[1], shape))
        return jnp.where(hit, 1.0, 0.0).astype(bf16)

    def column(v):
        return jnp.transpose(jnp.broadcast_to(v, (128, T)))[:, 0:1]

    def disp(e, k, d):
        return pltpu.make_async_remote_copy(
            src_ref=zs[k].at[e, d], dst_ref=zr[k].at[e, me], send_sem=ds_sem.at[e, k], recv_sem=dr_sem.at[e, k],
            device_id={"ep": d}, device_id_type=pl.DeviceIdType.MESH)

    def gather(e, k, mains, rems):
        k0, width = KS[k]
        w2 = width // 2
        z = dot(mains, x_v[:, pl.ds(k0, width)]).astype(bf16)
        zs[k][e, :, 0:16, :] = z[:, :w2].reshape(N, 16, w2)
        zs[k][e, :, 16:32, :] = z[:, w2:].reshape(N, 16, w2)
        z = dot(rems[0], x_v[:, pl.ds(k0, w2)]) + dot(rems[1], x_v[:, pl.ds(k0 + w2, w2)])
        zs[k][e, :, 32:40, :] = z.astype(bf16).reshape(N, 8, w2)

    for e in range(LOCAL):
        r = iota((N * 8, 1), 0)
        mains = pick(main_code(iota((N * MAIN, 1), 0), e))
        rems = [pick(rem_code(r, e, side)) for side in range(2)]
        if e == 0:
            x_copy.wait()
        for k in range(len(KS)):
            gather(e, k, mains, rems)
            if e == 0 and k == 0:
                pl.semaphore_wait(barrier, N - 1)
            for d in order:
                disp(e, k, d).start()
            zr[k][e, me] = zs[k][e, me]
            if e == 0:
                for g in range(RING):
                    wb_start(g, k)
    for c in range(len(CHUNKS)):
        wd_copy(0, c).start()

    un_r = iota((64, 128), 0)
    un_c = iota((64, 128), 1)
    unfold_l = jnp.where((un_r >> 2) * 8 + (un_r & 3) == un_c, 1.0, 0.0).astype(bf16)
    unfold_r = jnp.where((un_r >> 2) * 8 + (un_r & 3) + 4 == un_c, 1.0, 0.0).astype(bf16)

    col = [column(row[j]) for j in range(2)]
    weight = [column(gate[j:j + 1].astype(bf16).astype(f32)) for j in range(2)]

    def blend(code):
        shape = (T, code.shape[1])
        return sum(jnp.where(jnp.broadcast_to(col[j], shape) == jnp.broadcast_to(code, shape),
                             jnp.broadcast_to(weight[j], shape), 0.0) for j in range(2)).astype(bf16)

    for e in range(LOCAL):
        bm[e] = blend(main_code(iota((1, 256), 1), e))
        for side in range(2):
            br[e, side] = blend(rem_code(iota((1, 128), 1), e, side))

    def comb(e, c, d):
        return pltpu.make_async_remote_copy(
            src_ref=os[c].at[e, d], dst_ref=cr[c].at[e, me], send_sem=cs_sem.at[e, c], recv_sem=cr_sem.at[e, c],
            device_id={"ep": d}, device_id_type=pl.DeviceIdType.MESH)

    def landed(ref, sem):
        pltpu.make_async_copy(ref.at[pl.ds(0, N - 1)], ref.at[pl.ds(0, N - 1)], sem).wait()

    def arrive(e, k):
        k0, width = KS[k]
        w2 = width // 2
        landed(zr[k].at[e], dr_sem.at[e, k])
        lhs[0:256, pl.ds(k0, w2)] = zr[k][e, :, 0:16, :].reshape(N * 16, w2)
        lhs[0:256, pl.ds(k0 + w2, w2)] = zr[k][e, :, 16:32, :].reshape(N * 16, w2)
        rem = zr[k][e, :, 32:40, :].reshape(N * 8, w2)
        lhs[256:320, pl.ds(k0, w2)] = dot(unfold_l, rem).astype(bf16)
        lhs[256:320, pl.ds(k0 + w2, w2)] = dot(unfold_r, rem).astype(bf16)

    def finish(f, gu):
        h[:, pl.ds(pl.multiple_of(f * FT, FT), FT)] = (jax.nn.silu(gu[:, :FT]) * gu[:, FT:]).astype(bf16)

    def sweep(e, ks, tile):
        def group(f0, n):
            gs = [e * NF + f0 + t for t in range(n)]
            for g in gs:
                for k in ks:
                    wb_wait(g, k)
            for t, g in enumerate(gs):
                tile(f0 + t, g % RING)
            for g in gs:
                @pl.when(g + RING < LOCAL * NF)
                def _():
                    for k in ks:
                        wb_start(g + RING, k)

        @pl.loop(0, NF // GROUP)
        def _(i):
            group(i * GROUP, GROUP)

        group(NF // GROUP * GROUP, NF % GROUP)

    def first(f, s):
        acc[f] = dot(lhs[:, pl.ds(*KS[0])], wb[s, pl.ds(*KS[0]), :])

    def second(f, s):
        finish(f, acc[f] + dot(lhs[:, pl.ds(*KS[1])], wb[s, pl.ds(*KS[1]), :]))

    def whole(f, s):
        finish(f, dot(lhs[...], wb[s]))

    for e in range(LOCAL):
        if e == 0:
            arrive(e, 0)
            sweep(e, (0,), first)
            arrive(e, 1)
            sweep(e, (1,), second)
        else:
            arrive(e, 0)
            arrive(e, 1)
            sweep(e, (0, 1), whole)

        for c, (c0, width) in enumerate(CHUNKS):
            w2 = width // 2
            wd_copy(e, c).wait()
            out = dot(h[...], wd[:, pl.ds(c0, width)])
            if e + 1 < LOCAL:
                wd_copy(e + 1, c).start()
            main = out[0:256].astype(bf16)
            os[c][e, :, 0:16, :] = main[:, :w2].reshape(N, 16, w2)
            os[c][e, :, 16:32, :] = main[:, w2:].reshape(N, 16, w2)
            rem = out[256:320].reshape(N, 4, width)
            os[c][e, :, 32:40, :] = jnp.concatenate([rem[:, :, :w2], rem[:, :, w2:]], axis=1).astype(bf16)
            for d in order:
                comb(e, c, d).start()
            cr[c][e, me] = os[c][e, me]

    for c, (c0, width) in enumerate(CHUNKS):
        w2 = width // 2
        for e in range(LOCAL):
            landed(cr[c].at[e], cr_sem.at[e, c])
        for side in range(2):
            total = 0
            for e in range(LOCAL):
                total += dot(bm[e], cr[c][e, :, 16 * side:16 * side + 16, :].reshape(N * 16, w2))
                total += dot(br[e, side], cr[c][e, :, 32:40, :].reshape(N * 8, w2))
            y_ref[:, pl.ds(c0 + side * w2, w2)] = total.astype(bf16)

    for e in range(LOCAL):
        for k in range(len(KS)):
            landed(zs[k].at[e], ds_sem.at[e, k])
        for c in range(len(CHUNKS)):
            landed(os[c].at[e], cs_sem.at[e, c])


def solution(mesh):
    def body(x, expert, slot, gate, wg, wu, wd):
        vmem = pl.BlockSpec(memory_space=pltpu.VMEM)
        hbm = pl.BlockSpec(memory_space=pltpu.HBM)
        halves = [w // 2 for _, w in CHUNKS]
        y = pl.pallas_call(
            kernel,
            name="moe",
            out_shape=jax.ShapeDtypeStruct((T, D), bf16),
            in_specs=[hbm, vmem, vmem, vmem, hbm, hbm, hbm],
            out_specs=vmem,
            scratch_shapes=[
                pltpu.VMEM((T, D), bf16),
                *[pltpu.VMEM((LOCAL, N, 40, w // 2), bf16) for _, w in KS],
                *[pltpu.VMEM((LOCAL, N, 40, w // 2), bf16) for _, w in KS],
                pltpu.VMEM((N * SLOTS, D), bf16),
                pltpu.VMEM((NF, N * SLOTS, 2 * FT), f32),
                pltpu.VMEM((N * SLOTS, F), bf16),
                pltpu.VMEM((RING, D, 2 * FT), bf16),
                pltpu.VMEM((F, D), bf16),
                *[pltpu.VMEM((LOCAL, N, 40, w), bf16) for w in halves],
                *[pltpu.VMEM((LOCAL, N, 40, w), bf16) for w in halves],
                pltpu.VMEM((LOCAL, T, N * MAIN), bf16),
                pltpu.VMEM((LOCAL, 2, T, N * 8), bf16),
                pltpu.SemaphoreType.DMA,
                pltpu.SemaphoreType.DMA((len(KS), RING)),
                pltpu.SemaphoreType.DMA((len(CHUNKS),)),
                pltpu.SemaphoreType.DMA((LOCAL, len(KS))),
                pltpu.SemaphoreType.DMA((LOCAL, len(KS))),
                pltpu.SemaphoreType.DMA((LOCAL, len(CHUNKS))),
                pltpu.SemaphoreType.DMA((LOCAL, len(CHUNKS))),
            ],
            compiler_params=pltpu.CompilerParams(
                collective_id=0, has_side_effects=True, vmem_limit_bytes=VMEM_LIMIT),
        )(x[0, 0], expert[0, 0].T, slot[0, 0].T, gate[0, 0].T, wg, wu, wd)
        return y[None, None]

    tok, weights = P("dp", "ep", None, None), P("ep", None, None)
    return jax.shard_map(body, mesh=mesh, in_specs=(tok,) * 4 + (weights,) * 3, out_specs=tok, check_vma=False)
```

```python
import jax
import jax.numpy as jnp
from jax import lax
from jax.experimental import pallas as pl
from jax.experimental.pallas import tpu as pltpu
from jax.sharding import PartitionSpec as P

N = 16
LOCAL = 2
T, D, F = 256, 1792, 4864
SLOTS = 20
HALF = D // 2
FT = 256
NF = F // FT
RING, GROUP = 15, 5
AGAIN = NF - RING
assert AGAIN <= NF % GROUP
LOADS = NF + AGAIN
CHUNKS = ((0, 1024), (1024, 512), (1536, 256))
VMEM_LIMIT = 67_043_328
PART = ((0, 16), (16, 24))
SPAN = ((0, 128), (128, 192))
f32, bf16, i32 = jnp.float32, jnp.bfloat16, jnp.int32


def dot(a, b):
    return jnp.dot(a, b, preferred_element_type=f32)


def iota(shape, axis):
    return lax.broadcasted_iota(i32, shape, axis)


def code_of(r, e, side, rows, q0):
    d = {16: r >> 4, 24: (r * 2731) >> 16, 40: (r * 1639) >> 16}[rows]
    q = r - rows * d + q0
    early = q < 32
    half = jnp.where(early, (q >> 3) & 1, (q >> 2) & 1)
    place = jnp.where(early, ((q >> 4) << 3) + (q & 7), 16 + (q & 3))
    return jnp.where(half == side, (2 * d + e) * 32 + place, -2)


def kernel(x_hbm, expert, slot, gate, wg_hbm, wu_hbm, wd_hbm, y_hbm,
           x_v, zs0, zs1, zr0, zr1, lhs, h, wb, wd, os0, os1, os2, cr0, cr1, cr2, bl0, bl11, bl10, y_p,
           x_sem, y_sem, wb_sem, wd_sem, ds_sem, dr_sem, cs_sem, cr_sem):
    zs, zr = (zs0, zs1), (zr0, zr1)
    os, cr = (os0, os1, os2), (cr0, cr1, cr2)
    me = lax.axis_index("ep")
    bits = [(me // (1 << b)) % 2 for b in range(4)]

    def partner(k):
        return sum((1 - bits[b] if (k >> b) & 1 else bits[b]) * (1 << b) for b in range(4))

    order = [partner((7 * k) % 16) for k in range(1, N)]

    barrier = pltpu.get_barrier_semaphore()
    for d in order:
        pl.semaphore_signal(barrier, inc=1, device_id={"ep": d}, device_id_type=pl.DeviceIdType.MESH)
    x_copy = pltpu.make_async_copy(x_hbm, x_v, x_sem)
    x_copy.start()

    def wb_start(load):
        e, f, s = load // LOADS, load % LOADS % NF, load % RING
        cols = pl.ds(pl.multiple_of(f * FT, FT), FT)
        pltpu.make_async_copy(wg_hbm.at[e, :, cols], wb.at[s, :, pl.ds(0, FT)], wb_sem.at[s]).start()
        pltpu.make_async_copy(wu_hbm.at[e, :, cols], wb.at[s, :, pl.ds(FT, FT)], wb_sem.at[s]).start()

    def wb_wait(load):
        part = wb.at[load % RING]
        pltpu.make_async_copy(part, part, wb_sem.at[load % RING]).wait()

    def wd_copy(e, c):
        cols = pl.ds(*CHUNKS[c])
        return pltpu.make_async_copy(wd_hbm.at[e, :, cols], wd.at[:, cols], wd_sem.at[c])

    row = [jnp.where(slot[j:j + 1] < SLOTS, expert[j:j + 1] * 32 + slot[j:j + 1], -1) for j in range(2)]

    def pick(code):
        shape = (code.shape[0], T)
        hit = (jnp.broadcast_to(code, shape) == jnp.broadcast_to(row[0], shape)) | (
            jnp.broadcast_to(code, shape) == jnp.broadcast_to(row[1], shape))
        return jnp.where(hit, 1.0, 0.0).astype(bf16)

    def column(v):
        return jnp.transpose(jnp.broadcast_to(v, (128, T)))[:, 0:1]

    def disp(e, p, d):
        return pltpu.make_async_remote_copy(
            src_ref=zs[p].at[e, d], dst_ref=zr[p].at[e, me], send_sem=ds_sem.at[e, p], recv_sem=dr_sem.at[e, p],
            device_id={"ep": d}, device_id_type=pl.DeviceIdType.MESH)

    for e, p in ((0, 0), (0, 1), (1, 1), (1, 0)):
        q0, rows = PART[p]
        r = iota((N * rows, 1), 0)
        picks = [pick(code_of(r, e, side, rows, q0)) for side in range(2)]
        if (e, p) == (0, 0):
            x_copy.wait()
            for load in range(RING):
                wb_start(load)
        z = dot(picks[0], x_v[:, :HALF]) + dot(picks[1], x_v[:, HALF:])
        zs[p][e] = z.astype(bf16).reshape(N, rows, HALF)
        if (e, p) == (0, 0):
            pl.semaphore_wait(barrier, N - 1)
        for d in order:
            disp(e, p, d).start()
        zr[p][e, me] = zs[p][e, me]

    un_r = iota((64, 128), 0)
    un_c = iota((64, 128), 1)
    unfold = [jnp.where((un_r >> 2) * 8 + (un_r & 3) + 4 * side == un_c, 1.0, 0.0).astype(bf16) for side in range(2)]

    col = [column(row[j]) for j in range(2)]
    weight = [column(gate[j:j + 1].astype(bf16).astype(f32)) for j in range(2)]

    for ref, e, q0, rows in ((bl0, 0, 0, 40), (bl11, 1, *PART[1]), (bl10, 1, *PART[0])):
        for side in range(2):
            code = code_of(iota((1, N * rows), 1), e, side, rows, q0)
            shape = (T, N * rows)
            ref[side] = sum(jnp.where(jnp.broadcast_to(col[j], shape) == jnp.broadcast_to(code, shape),
                                      jnp.broadcast_to(weight[j], shape), 0.0) for j in range(2)).astype(bf16)

    def block_rows(e, p):
        return (0, pl.ds(0, 40)) if e == 0 else (1 + p, pl.ds(*PART[p]))

    def comb(e, p, c, d):
        i, rows = block_rows(e, p)
        return pltpu.make_async_remote_copy(
            src_ref=os[c].at[e, d, rows], dst_ref=cr[c].at[e, me, rows], send_sem=cs_sem.at[i, c],
            recv_sem=cr_sem.at[i, c], device_id={"ep": d}, device_id_type=pl.DeviceIdType.MESH)

    def landed(ref, sem):
        pltpu.make_async_copy(ref.at[pl.ds(0, N - 1)], ref.at[pl.ds(0, N - 1)], sem).wait()

    def arrive(e, p):
        m0 = SPAN[p][0]
        landed(zr[p].at[e], dr_sem.at[e, p])
        for side in range(2):
            cols = pl.ds(side * HALF, HALF)
            lhs[m0:m0 + 128, cols] = zr[p][e, :, 8 * side:8 * side + 8, :].reshape(N * 8, HALF)
            if p == 1:
                lhs[256:320, cols] = dot(unfold[side], zr[p][e, :, 16:24, :].reshape(N * 8, HALF)).astype(bf16)

    def sweep(e, p, again):
        first = e * LOADS + (AGAIN if again else 0)
        rows = pl.ds(*SPAN[p])

        def arrived(load0, n):
            for t in range(n):
                wb_wait(load0 + t)

        def multiply(load0, n):
            for t in range(n):
                load = load0 + t
                gu = dot(lhs[rows, :], wb[load % RING])
                f = load % LOADS % NF
                h[rows, pl.ds(pl.multiple_of(f * FT, FT), FT)] = (jax.nn.silu(gu[:, :FT]) * gu[:, FT:]).astype(bf16)

        def refill(load0, n):
            for t in range(n):
                wb_start(load0 + t + RING)

        if not again:
            arrived(first, GROUP)
        multiply(first, GROUP)
        refill(first, AGAIN)
        if again and e == 0:
            for c in range(1, len(CHUNKS)):
                wd_copy(0, c).start()

        @pl.loop(1, NF // GROUP)
        def _(i):
            load0 = first + i * GROUP
            if not again:
                arrived(load0, GROUP)
            multiply(load0, GROUP)
            if again and e + 1 < LOCAL:
                for t in range(GROUP):
                    load = load0 - GROUP + t

                    @pl.when(load >= first + AGAIN)
                    def _():
                        wb_start(load + RING)

        n = NF % GROUP
        load0 = first + NF - n
        arrived(load0 + n - AGAIN if again else load0, AGAIN if again else n)
        if not again:
            for c in range(1) if e == 0 else range(1, len(CHUNKS)):
                wd_copy(e, c).start()
        multiply(load0, n)
        if again and e + 1 < LOCAL:
            refill(load0 - GROUP, GROUP + n)

    def down(e, parts):
        m0, m1 = SPAN[parts[0]][0], sum(SPAN[parts[-1]])
        for c, (c0, width) in enumerate(CHUNKS):
            w2 = width // 2
            if parts[0] == 0 and e == 0 or parts[0] == 1:
                wd_copy(e, c).wait()
            if width == 256:
                k = 2560
                y_p[0:m1 - m0, 0:width] = dot(h[m0:m1, :k], wd[:k, pl.ds(c0, width)])
                out = y_p[0:m1 - m0, 0:width] + dot(h[m0:m1, k:], wd[k:, pl.ds(c0, width)])
            else:
                out = dot(h[m0:m1, :], wd[:, pl.ds(c0, width)])
            for p in parts:
                q0, base = PART[p][0], SPAN[p][0] - m0
                for side in range(2):
                    half = out[base:base + 128, side * w2:side * w2 + w2].astype(bf16)
                    os[c][e, :, q0 + 8 * side:q0 + 8 * side + 8, :] = half.reshape(N, 8, w2)
                if p == 1:
                    rem = out[base + 128:base + 192].reshape(N, 4, width)
                    os[c][e, :, 32:40, :] = jnp.concatenate([rem[:, :, :w2], rem[:, :, w2:]], axis=1).astype(bf16)
            for d in order:
                comb(e, parts[0], c, d).start()
            own = block_rows(e, parts[0])[1]
            cr[c][e, me, own] = os[c][e, me, own]
        if e + 1 < LOCAL:
            wd_copy(e + 1, 0).start()

    arrive(0, 0)
    sweep(0, 0, False)
    arrive(0, 1)
    sweep(0, 1, True)
    down(0, (0, 1))
    arrive(1, 1)
    sweep(1, 1, False)
    down(1, (1,))
    arrive(1, 0)
    sweep(1, 0, True)
    down(1, (0,))

    def y_copy(c):
        cols = pl.ds(*CHUNKS[c])
        return pltpu.make_async_copy(x_v.at[:, cols], y_hbm.at[:, cols], y_sem.at[c])

    late = pl.ds(*PART[0])

    def wait_for(e, p, c):
        i, rows = block_rows(e, p)
        landed(cr[c].at[e, :, rows], cr_sem.at[i, c])

    for c, (c0, width) in enumerate(CHUNKS):
        w2 = width // 2
        wait_for(0, 0, c)
        wait_for(1, 1, c)
        for side in range(2):
            y_p[0:T, pl.ds(c0 + side * w2, w2)] = dot(bl0[side], cr[c][0].reshape(N * 40, w2)) + dot(
                bl11[side], cr[c][1, :, pl.ds(*PART[1]), :].reshape(N * 24, w2))
    for c, (c0, width) in enumerate(CHUNKS):
        w2 = width // 2
        wait_for(1, 0, c)
        for side in range(2):
            cols = pl.ds(c0 + side * w2, w2)
            x_v[:, cols] = (y_p[0:T, cols] + dot(bl10[side], cr[c][1, :, late, :].reshape(N * 16, w2))).astype(bf16)
        y_copy(c).start()

    for e in range(LOCAL):
        for p in range(2):
            landed(zs[p].at[e], ds_sem.at[e, p])
    for c in range(len(CHUNKS)):
        for e, p in ((0, 0), (1, 1), (1, 0)):
            i, rows = block_rows(e, p)
            landed(os[c].at[e, :, rows], cs_sem.at[i, c])
        y_copy(c).wait()


def solution(mesh):
    def body(x, expert, slot, gate, wg, wu, wd):
        vmem = pl.BlockSpec(memory_space=pltpu.VMEM)
        hbm = pl.BlockSpec(memory_space=pltpu.HBM)
        halves = [w // 2 for _, w in CHUNKS]
        dma = pltpu.SemaphoreType.DMA
        y = pl.pallas_call(
            kernel,
            name="moe",
            out_shape=jax.ShapeDtypeStruct((T, D), bf16),
            in_specs=[hbm, vmem, vmem, vmem, hbm, hbm, hbm],
            out_specs=hbm,
            scratch_shapes=[
                pltpu.VMEM((T, D), bf16),
                *[pltpu.VMEM((LOCAL, N, rows, HALF), bf16) for _, rows in PART],
                *[pltpu.VMEM((LOCAL, N, rows, HALF), bf16) for _, rows in PART],
                pltpu.VMEM((N * SLOTS, D), bf16),
                pltpu.VMEM((N * SLOTS, F), bf16),
                pltpu.VMEM((RING, D, 2 * FT), bf16),
                pltpu.VMEM((F, D), bf16),
                *[pltpu.VMEM((LOCAL, N, 40, w), bf16) for w in halves],
                *[pltpu.VMEM((LOCAL, N, 40, w), bf16) for w in halves],
                *[pltpu.VMEM((2, T, N * rows), bf16) for rows in (40, 24, 16)],
                pltpu.VMEM((N * SLOTS, D), f32),
                dma,
                dma((len(CHUNKS),)),
                dma((RING,)),
                dma((len(CHUNKS),)),
                dma((LOCAL, 2)),
                dma((LOCAL, 2)),
                dma((3, len(CHUNKS))),
                dma((3, len(CHUNKS))),
            ],
            compiler_params=pltpu.CompilerParams(
                collective_id=0, has_side_effects=True, vmem_limit_bytes=VMEM_LIMIT),
        )(x[0, 0], expert[0, 0].T, slot[0, 0].T, gate[0, 0].T, wg, wu, wd)
        return y[None, None]

    tok, weights = P("dp", "ep", None, None), P("ep", None, None)
    return jax.shard_map(body, mesh=mesh, in_specs=(tok,) * 4 + (weights,) * 3, out_specs=tok, check_vma=False)
```

```python
import jax
import jax.numpy as jnp
from jax import lax
from jax.experimental import pallas as pl
from jax.experimental.pallas import tpu as pltpu
from jax.sharding import PartitionSpec as P

N = 16
LOCAL = 2
T, D, F = 256, 1792, 4864
SLOTS = 20
HALF = D // 2
FT = 256
NF = F // FT
RING, GROUP = 15, 5
AGAIN = NF - RING
assert AGAIN <= NF % GROUP
LOADS = NF + AGAIN
CHUNKS = ((0, 1024), (1024, 512), (1536, 256))
VMEM_LIMIT = 67_043_328
PART = ((0, 16), (16, 24))
SPAN = ((0, 128), (128, 192))
f32, bf16, i32 = jnp.float32, jnp.bfloat16, jnp.int32


def dot(a, b):
    return jnp.dot(a, b, preferred_element_type=f32)


def iota(shape, axis):
    return lax.broadcasted_iota(i32, shape, axis)


def code_of(r, e, side, rows, q0):
    d = {16: r >> 4, 24: (r * 2731) >> 16, 40: (r * 1639) >> 16}[rows]
    q = r - rows * d + q0
    early = q < 32
    half = jnp.where(early, (q >> 3) & 1, (q >> 2) & 1)
    place = jnp.where(early, ((q >> 4) << 3) + (q & 7), 16 + (q & 3))
    return jnp.where(half == side, (2 * d + e) * 32 + place, -2)


def kernel(x_hbm, expert_hbm, slot_hbm, gate_hbm, wg_hbm, wu_hbm, wd_hbm, y_hbm,
           expert, slot, gate, x_v, zs0, zs1, zr0, zr1, lhs, h, wb, wd, os0, os1, os2, cr0, cr1, cr2, bl0, bl11, bl10, y_p,
           in_sem, x_sem, y_sem, wb_sem, wd_sem, ds_sem, dr_sem, cs_sem, cr_sem):
    zs, zr = (zs0, zs1), (zr0, zr1)
    os, cr = (os0, os1, os2), (cr0, cr1, cr2)
    me = lax.axis_index("ep")
    bits = [(me // (1 << b)) % 2 for b in range(4)]

    def partner(k):
        return sum((1 - bits[b] if (k >> b) & 1 else bits[b]) * (1 << b) for b in range(4))

    order = [partner(k) for k in (14, 6, 2, 12, 4, 10, 8, 15, 7, 3, 13, 5, 11, 9, 1)]

    barrier = pltpu.get_barrier_semaphore()
    for d in order:
        pl.semaphore_signal(barrier, inc=1, device_id={"ep": d}, device_id_type=pl.DeviceIdType.MESH)
    small = [pltpu.make_async_copy(src, dst, in_sem.at[i]) for i, (src, dst) in enumerate(
        ((expert_hbm, expert), (slot_hbm, slot), (gate_hbm, gate)))]
    for copy in small:
        copy.start()
    x_copy = pltpu.make_async_copy(x_hbm, x_v, x_sem)
    x_copy.start()

    def wb_start(load):
        e, f, s = load // LOADS, load % LOADS % NF, load % RING
        cols = pl.ds(pl.multiple_of(f * FT, FT), FT)
        pltpu.make_async_copy(wg_hbm.at[e, :, cols], wb.at[s, :, pl.ds(0, FT)], wb_sem.at[s]).start()
        pltpu.make_async_copy(wu_hbm.at[e, :, cols], wb.at[s, :, pl.ds(FT, FT)], wb_sem.at[s]).start()

    def wb_wait(load):
        part = wb.at[load % RING]
        pltpu.make_async_copy(part, part, wb_sem.at[load % RING]).wait()

    def wd_copy(e, c):
        cols = pl.ds(*CHUNKS[c])
        return pltpu.make_async_copy(wd_hbm.at[e, :, cols], wd.at[:, cols], wd_sem.at[c])

    for copy in small:
        copy.wait()
    row = [jnp.where(slot[j:j + 1] < SLOTS, expert[j:j + 1] * 32 + slot[j:j + 1], -1) for j in range(2)]

    def pick(code):
        shape = (code.shape[0], T)
        hit = (jnp.broadcast_to(code, shape) == jnp.broadcast_to(row[0], shape)) | (
            jnp.broadcast_to(code, shape) == jnp.broadcast_to(row[1], shape))
        return jnp.where(hit, 1.0, 0.0).astype(bf16)

    def column(v):
        return jnp.transpose(jnp.broadcast_to(v, (128, T)))[:, 0:1]

    def disp(e, p, d):
        return pltpu.make_async_remote_copy(
            src_ref=zs[p].at[e, d], dst_ref=zr[p].at[e, me], send_sem=ds_sem.at[e, p], recv_sem=dr_sem.at[e, p],
            device_id={"ep": d}, device_id_type=pl.DeviceIdType.MESH)

    for e, p in ((0, 0), (0, 1), (1, 1), (1, 0)):
        q0, rows = PART[p]
        r = iota((N * rows, 1), 0)
        picks = [pick(code_of(r, e, side, rows, q0)) for side in range(2)]
        if (e, p) == (0, 0):
            x_copy.wait()
            for load in range(RING):
                wb_start(load)
        z = dot(picks[0], x_v[:, :HALF]) + dot(picks[1], x_v[:, HALF:])
        zs[p][e] = z.astype(bf16).reshape(N, rows, HALF)
        if (e, p) == (0, 0):
            pl.semaphore_wait(barrier, N - 1)
        for d in order:
            disp(e, p, d).start()
        zr[p][e, me] = zs[p][e, me]

    un_r = iota((64, 128), 0)
    un_c = iota((64, 128), 1)
    unfold = [jnp.where((un_r >> 2) * 8 + (un_r & 3) + 4 * side == un_c, 1.0, 0.0).astype(bf16) for side in range(2)]

    col = [column(row[j]) for j in range(2)]
    weight = [column(gate[j:j + 1].astype(bf16).astype(f32)) for j in range(2)]

    for ref, e, q0, rows in ((bl0, 0, 0, 40), (bl11, 1, *PART[1]), (bl10, 1, *PART[0])):
        for side in range(2):
            code = code_of(iota((1, N * rows), 1), e, side, rows, q0)
            shape = (T, N * rows)
            ref[side] = sum(jnp.where(jnp.broadcast_to(col[j], shape) == jnp.broadcast_to(code, shape),
                                      jnp.broadcast_to(weight[j], shape), 0.0) for j in range(2)).astype(bf16)

    def block_rows(e, p):
        return (0, pl.ds(0, 40)) if e == 0 else (1 + p, pl.ds(*PART[p]))

    def comb(e, p, c, d):
        i, rows = block_rows(e, p)
        return pltpu.make_async_remote_copy(
            src_ref=os[c].at[e, d, rows], dst_ref=cr[c].at[e, me, rows], send_sem=cs_sem.at[i, c],
            recv_sem=cr_sem.at[i, c], device_id={"ep": d}, device_id_type=pl.DeviceIdType.MESH)

    def landed(ref, sem):
        pltpu.make_async_copy(ref.at[pl.ds(0, N - 1)], ref.at[pl.ds(0, N - 1)], sem).wait()

    def arrive(e, p):
        m0 = SPAN[p][0]
        landed(zr[p].at[e], dr_sem.at[e, p])
        for side in range(2):
            cols = pl.ds(side * HALF, HALF)
            lhs[m0:m0 + 128, cols] = zr[p][e, :, 8 * side:8 * side + 8, :].reshape(N * 8, HALF)
            if p == 1:
                lhs[256:320, cols] = dot(unfold[side], zr[p][e, :, 16:24, :].reshape(N * 8, HALF)).astype(bf16)

    def sweep(e, p, again):
        first = e * LOADS + (AGAIN if again else 0)
        rows = pl.ds(*SPAN[p])

        def arrived(load0, n):
            for t in range(n):
                wb_wait(load0 + t)

        def multiply(load0, n):
            for t in range(n):
                load = load0 + t
                gu = dot(lhs[rows, :], wb[load % RING])
                f = load % LOADS % NF
                h[rows, pl.ds(pl.multiple_of(f * FT, FT), FT)] = (jax.nn.silu(gu[:, :FT]) * gu[:, FT:]).astype(bf16)

        def refill(load0, n):
            for t in range(n):
                wb_start(load0 + t + RING)

        if not again:
            arrived(first, GROUP)
        multiply(first, GROUP)
        refill(first, AGAIN)
        if again and e == 0:
            for c in range(1, len(CHUNKS)):
                wd_copy(0, c).start()

        @pl.loop(1, NF // GROUP)
        def _(i):
            load0 = first + i * GROUP
            if not again:
                arrived(load0, GROUP)
            multiply(load0, GROUP)
            if again and e + 1 < LOCAL:
                for t in range(GROUP):
                    load = load0 - GROUP + t

                    @pl.when(load >= first + AGAIN)
                    def _():
                        wb_start(load + RING)

        n = NF % GROUP
        load0 = first + NF - n
        arrived(load0 + n - AGAIN if again else load0, AGAIN if again else n)
        if not again:
            for c in range(1) if e == 0 else range(1, len(CHUNKS)):
                wd_copy(e, c).start()
        multiply(load0, n)
        if again and e + 1 < LOCAL:
            refill(load0 - GROUP, GROUP + n)

    def down(e, parts):
        m0, m1 = SPAN[parts[0]][0], sum(SPAN[parts[-1]])
        for c, (c0, width) in enumerate(CHUNKS):
            w2 = width // 2
            if parts[0] == 0 and e == 0 or parts[0] == 1:
                wd_copy(e, c).wait()
            if width == 256:
                k = 2560
                y_p[0:m1 - m0, 0:width] = dot(h[m0:m1, :k], wd[:k, pl.ds(c0, width)])
                out = y_p[0:m1 - m0, 0:width] + dot(h[m0:m1, k:], wd[k:, pl.ds(c0, width)])
            else:
                out = dot(h[m0:m1, :], wd[:, pl.ds(c0, width)])
            for p in parts:
                q0, base = PART[p][0], SPAN[p][0] - m0
                for side in range(2):
                    half = out[base:base + 128, side * w2:side * w2 + w2].astype(bf16)
                    os[c][e, :, q0 + 8 * side:q0 + 8 * side + 8, :] = half.reshape(N, 8, w2)
                if p == 1:
                    rem = out[base + 128:base + 192].reshape(N, 4, width)
                    os[c][e, :, 32:40, :] = jnp.concatenate([rem[:, :, :w2], rem[:, :, w2:]], axis=1).astype(bf16)
            for d in order:
                comb(e, parts[0], c, d).start()
            own = block_rows(e, parts[0])[1]
            cr[c][e, me, own] = os[c][e, me, own]
        if e + 1 < LOCAL:
            wd_copy(e + 1, 0).start()

    arrive(0, 0)
    sweep(0, 0, False)
    arrive(0, 1)
    sweep(0, 1, True)
    down(0, (0, 1))
    arrive(1, 1)
    sweep(1, 1, False)
    down(1, (1,))
    arrive(1, 0)
    sweep(1, 0, True)
    down(1, (0,))

    def y_copy(c):
        cols = pl.ds(*CHUNKS[c])
        return pltpu.make_async_copy(x_v.at[:, cols], y_hbm.at[:, cols], y_sem.at[c])

    late = pl.ds(*PART[0])

    def wait_for(e, p, c):
        i, rows = block_rows(e, p)
        landed(cr[c].at[e, :, rows], cr_sem.at[i, c])

    for c, (c0, width) in enumerate(CHUNKS):
        w2 = width // 2
        wait_for(0, 0, c)
        wait_for(1, 1, c)
        for side in range(2):
            y_p[0:T, pl.ds(c0 + side * w2, w2)] = dot(bl0[side], cr[c][0].reshape(N * 40, w2)) + dot(
                bl11[side], cr[c][1, :, pl.ds(*PART[1]), :].reshape(N * 24, w2))
    for c, (c0, width) in enumerate(CHUNKS):
        w2 = width // 2
        wait_for(1, 0, c)
        for side in range(2):
            cols = pl.ds(c0 + side * w2, w2)
            x_v[:, cols] = (y_p[0:T, cols] + dot(bl10[side], cr[c][1, :, late, :].reshape(N * 16, w2))).astype(bf16)
        y_copy(c).start()

    for e in range(LOCAL):
        for p in range(2):
            landed(zs[p].at[e], ds_sem.at[e, p])
    for c in range(len(CHUNKS)):
        for e, p in ((0, 0), (1, 1), (1, 0)):
            i, rows = block_rows(e, p)
            landed(os[c].at[e, :, rows], cs_sem.at[i, c])
        y_copy(c).wait()


def solution(mesh):
    def body(x, expert, slot, gate, wg, wu, wd):
        hbm = pl.BlockSpec(memory_space=pltpu.HBM)
        halves = [w // 2 for _, w in CHUNKS]
        dma = pltpu.SemaphoreType.DMA
        y = pl.pallas_call(
            kernel,
            name="moe",
            out_shape=jax.ShapeDtypeStruct((T, D), bf16),
            in_specs=[hbm] * 7,
            out_specs=hbm,
            scratch_shapes=[
                *[pltpu.VMEM((2, T), t) for t in (i32, i32, f32)],
                pltpu.VMEM((T, D), bf16),
                *[pltpu.VMEM((LOCAL, N, rows, HALF), bf16) for _, rows in PART],
                *[pltpu.VMEM((LOCAL, N, rows, HALF), bf16) for _, rows in PART],
                pltpu.VMEM((N * SLOTS, D), bf16),
                pltpu.VMEM((N * SLOTS, F), bf16),
                pltpu.VMEM((RING, D, 2 * FT), bf16),
                pltpu.VMEM((F, D), bf16),
                *[pltpu.VMEM((LOCAL, N, 40, w), bf16) for w in halves],
                *[pltpu.VMEM((LOCAL, N, 40, w), bf16) for w in halves],
                *[pltpu.VMEM((2, T, N * rows), bf16) for rows in (40, 24, 16)],
                pltpu.VMEM((N * SLOTS, D), f32),
                dma((3,)),
                dma,
                dma((len(CHUNKS),)),
                dma((RING,)),
                dma((len(CHUNKS),)),
                dma((LOCAL, 2)),
                dma((LOCAL, 2)),
                dma((3, len(CHUNKS))),
                dma((3, len(CHUNKS))),
            ],
            compiler_params=pltpu.CompilerParams(
                collective_id=0, has_side_effects=True, vmem_limit_bytes=VMEM_LIMIT),
        )(x[0, 0], expert[0, 0].T, slot[0, 0].T, gate[0, 0].T, wg, wu, wd)
        return y[None, None]

    tok, weights = P("dp", "ep", None, None), P("ep", None, None)
    return jax.shard_map(body, mesh=mesh, in_specs=(tok,) * 4 + (weights,) * 3, out_specs=tok, check_vma=False)
```
